128 devices in a mesh: gx: 8 (over x, core), gy: 16 (over z, y).
Axes of the slice: x: 4, y: 4, z: 4, core: 2. Of those that a mesh axis runs over, the one named last changes fastest.
Arguments:
- mask_feats: bfloat16 [256, 8, 14, 14, 256], P(('gx', 'gy')), may hold values from -6 to 6
- mask_cot: bfloat16 [256, 8, 14, 14, 256], P(('gx', 'gy')), may hold values from -6 to 6
- roi_counts: int32 [256], P(('gx', 'gy')), may hold values from 1 to 8, as said below
- rpn_feats: bfloat16 [256, 48, 32, 256], P(('gx', 'gy')), may hold values from -6 to 6
- rpn_cot: bfloat16 [256, 48, 32, 256], P(('gx', 'gy')), may hold values from -360 to 360
- anchor_counts: int32 [256], P(('gx', 'gy')), may hold values from 32 to 223
- mask_weight: float32 [2304, 256], replicated, may hold values from -0.125 to 0.125
- rpn_weight: float32 [2304, 256], replicated, may hold values from -0.125 to 0.125
- mask_moment: float32 [2304, 256], replicated, may hold values from -6 to 6
- rpn_moment: float32 [2304, 256], replicated, may hold values from -6 to 6
Outputs:
- new_mask_weight: float32 [2304, 256], replicated
- new_rpn_weight: float32 [2304, 256], replicated
- new_mask_moment: float32 [2304, 256], replicated
- new_rpn_moment: float32 [2304, 256], replicated
The draws below stay inside these ranges and needn't reach their ends.
Inputs may be any that keep to these rules, and one draw needn't show every extreme that they name: `roi_counts`: every image has at least one positive ROI; some image has all 8 slots positive.
All inputs are finite; a program needn't handle non-finite values.
Results may differ from the reference program's by a relative error of at most 0.0003.
Values sent between devices are 32-bit elements; how exact they have to be, the bound alone decides.
No kernel may reach another device: no remote copies, remote signals or barrier semaphores. Data moves between devices by JAX's collectives and lax.ppermute only.
A program may use at most 128 MiB of HBM per device.

```python
import jax
import jax.numpy as jnp
from jax import lax

C = 256
MH = 14
ROI_IMG = 8
IMG_DEV = 2
GH = 48
GW = 32
IMAGES = 256
N_GX = 8
N_GY = 16


def rising_level():
    image = jnp.arange(IMAGES, dtype=jnp.int32)
    device = image // IMG_DEV
    x_index = device // N_GY
    y_index = device % N_GY
    x_span = max(N_GX - 1, 1)
    y_span = max(N_GY - 1, 1)
    numer = x_index * y_span + y_index * x_span
    denom = 2 * x_span * y_span
    return (image, numer, denom)


def draw_roi_counts(key, part):
    image, numer, denom = rising_level()
    lowest = 1 + ROI_IMG * 5 // 8 * numer // denom
    extra = jax.random.randint(jax.random.fold_in(key, 11), (IMAGES,), 0, 3)
    counts = jnp.minimum(lowest + extra, ROI_IMG)
    counts = jnp.where(image == IMAGES - 1, ROI_IMG, counts)
    return counts.astype(jnp.int32)


def draw_anchor_counts(key, part):
    image, numer, denom = rising_level()
    lowest = 32 + 96 * numer // denom
    extra = jax.random.randint(jax.random.fold_in(key, 23), (IMAGES,), 0, 96)
    return (lowest + extra).astype(jnp.int32)


def level_of(own_key, shape, cuts, least, largest):
    gain = 1.0
    for axis_at, shards_of in cuts:
        draws = jax.random.uniform(jax.random.fold_in(jax.random.fold_in(own_key, 6), axis_at), (shards_of,), jnp.float32, least / len(cuts), largest / len(cuts))
        gain = gain * jnp.repeat(jnp.exp(draws), shape[axis_at] // shards_of).reshape((-1,) + (1,) * (len(shape) - 1 - axis_at))
    return gain


def bell_draw(key, shape, spread, limit, pieces=(), held_as=jnp.bfloat16):
    loudness = level_of(key, shape, pieces, -0.22, 0.18) if pieces else 1.0
    result = jax.random.normal(key, shape, jnp.float32) * spread * loudness
    return jnp.minimum(jnp.maximum(result, -limit), limit).astype(held_as)


def setup_inputs(seed: int = 0) -> dict:
    key_list = jax.random.split(jax.random.key(seed), 11)
    return {
        "mask_feats": bell_draw(key_list[0], (IMAGES, ROI_IMG, MH, MH, C), 1.0, 6.0, ((0, 128),)),
        "mask_cot": bell_draw(key_list[1], (IMAGES, ROI_IMG, MH, MH, C), 1.0, 6.0, ((0, 128),)),
        "roi_counts": draw_roi_counts(jax.random.fold_in(key_list[10], 71), 0),
        "rpn_feats": bell_draw(key_list[3], (IMAGES, GH, GW, C), 1.0, 6.0, ((0, 128),)),
        "rpn_cot": bell_draw(key_list[4], (IMAGES, GH, GW, C), 60.0, 360.0, ((0, 128),)),
        "anchor_counts": draw_anchor_counts(jax.random.fold_in(key_list[10], 71), 0),
        "mask_weight": bell_draw(key_list[6], (9 * C, C), (9 * C) ** -0.5, 0.125, (), jnp.float32),
        "rpn_weight": bell_draw(key_list[7], (9 * C, C), (9 * C) ** -0.5, 0.125, (), jnp.float32),
        "mask_moment": bell_draw(key_list[8], (9 * C, C), 1.0, 6.0, (), jnp.float32),
        "rpn_moment": bell_draw(key_list[9], (9 * C, C), 1.0, 6.0, (), jnp.float32),
    }


def weight_grad(feats, cotan):
    grid_rows = feats.shape[1]
    grid_cols = feats.shape[2]
    chans = feats.shape[3]
    padded = jnp.pad(feats, ((0, 0), (1, 1), (1, 1), (0, 0)))
    flat_cot = cotan.reshape(-1, chans)
    blocks = []
    for row_tap in range(3):
        for col_tap in range(3):
            window = padded[:, row_tap:row_tap + grid_rows, col_tap:col_tap + grid_cols, :].reshape(-1, chans)
            blocks.append(lax.dot_general(window, flat_cot, (((0,), (0,)), ((), ())), preferred_element_type=jnp.float32))
    return jnp.concatenate(blocks, axis=0)

def reference(mask_feats, mask_cot, roi_counts, rpn_feats, rpn_cot, anchor_counts, mask_weight, rpn_weight, mask_moment, rpn_moment):
    roi_total = jnp.sum(roi_counts).astype(jnp.float32)
    anchor_total = jnp.sum(anchor_counts).astype(jnp.float32)
    slots = jnp.arange(ROI_IMG, dtype=jnp.int32)
    valid_slots = (slots[None, :] < roi_counts[:, None]).astype(jnp.bfloat16)
    masked = mask_cot * valid_slots[:, :, None, None, None]
    mask_grad = weight_grad(mask_feats.reshape(-1, MH, MH, C), masked.reshape(-1, MH, MH, C)) / roi_total
    rpn_grad = weight_grad(rpn_feats, rpn_cot) / anchor_total
    new_mask_moment = 0.9 * mask_moment + mask_grad
    new_rpn_moment = 0.9 * rpn_moment + rpn_grad
    new_mask_weight = mask_weight - 0.02 * new_mask_moment
    new_rpn_weight = rpn_weight - 0.02 * new_rpn_moment
    return (new_mask_weight, new_rpn_weight, new_mask_moment, new_rpn_moment)
```

```python
import functools

import jax
import jax.numpy as jnp
from jax import lax
from jax.experimental import pallas as pl
from jax.experimental.pallas import tpu as pltpu
from jax.sharding import PartitionSpec as P


AXES = ("gx", "gy")
DEVICES = 128
C = 256
SUB = 32
ORDERS = ("xyz", "yzx", "zxy")
VM = pltpu.VMEM


def coords(i):
    return {"x": i // 32, "core": (i // 16) % 2, "z": (i // 4) % 4, "y": i % 4}


def linear(d):
    return d["x"] * 32 + d["core"] * 16 + d["z"] * 4 + d["y"]


def partner(i, axis, step):
    d = coords(i)
    if axis == "core":
        d["core"] ^= 1
    else:
        d[axis] ^= 1 if step == d["core"] else 3
    return linear(d)


def swap(v, axis, step=0):
    return lax.ppermute(v, AXES, [(i, partner(i, axis, step)) for i in range(DEVICES)])


def block_id(axis):
    gx, gy = lax.axis_index("gx"), lax.axis_index("gy")
    core = gx % 2
    at = {"x": gx // 2, "z": gy // 4, "y": gy % 4}[axis]
    high = at // 2
    gray = (high + at) % 2
    one, two = gray * 2 + high, high * 2 + gray
    return core * 4, (1 - core) * 4, jnp.where(core == 0, one, two), jnp.where(core == 0, two, one)


def rows_of(where, q):
    base, partner_base, low, partner_low = where
    own = pl.multiple_of((base + (low ^ q)) * SUB, SUB)
    other = pl.multiple_of((partner_base + (partner_low ^ q)) * SUB, SUB)
    return pl.ds(own, SUB), pl.ds(other, SUB)


def put(buf, grad, where, keep, send, slot):
    buf[...] = grad
    for q in range(4):
        own, other = rows_of(where, q)
        keep[q, pl.ds(slot * SUB, SUB), :] = buf[own, :]
        send[q, pl.ds(slot * SUB, SUB), :] = buf[other, :]


def dot_t(a, b):
    return lax.dot_general(a, b, (((0,), (0,)), ((), ())), preferred_element_type=jnp.float32)


def mask_kernel(roi, anchor, x, y, keep_a, send_a, keep_b, send_b, xp, yp, gbuf):
    row = 14 * 8
    zero = jnp.zeros((row, C), jnp.bfloat16)
    for b in range(3):
        for j in (0, 15, 30):
            xp[b, j * row : (j + 1) * row, :] = zero
    yp[14 * row : 15 * row, :] = zero
    slot = lax.broadcasted_iota(jnp.int32, (row, C), 0) % 8
    edge = jnp.zeros((8, C), jnp.bfloat16)
    for i in range(2):
        live = slot < roi[i]
        for r in range(14):
            v = x[i, r]
            at = (i * 15 + r + 1) * row
            xp[0, at : at + row, :] = jnp.concatenate([edge, v[: row - 8]], 0)
            xp[1, at : at + row, :] = v
            xp[2, at : at + row, :] = jnp.concatenate([v[8:], edge], 0)
            yp[at - row : at, :] = jnp.where(live, y[i, r], zero)
    where_a = block_id("x")
    where_b = block_id("y")
    for a in range(3):
        for b in range(3):
            t = 3 * a + b
            g = dot_t(xp[b, a * row : (a + 29) * row, :], yp[...])
            if t < 6:
                put(gbuf, g, where_a, keep_a, send_a, t)
            else:
                put(gbuf, g, where_b, keep_b, send_b, t - 6)
    lane = lax.broadcasted_iota(jnp.int32, (8, C), 1)
    rois = (roi[0] + roi[1]).astype(jnp.float32)
    anchors = (anchor[0] + anchor[1]).astype(jnp.float32)
    counts = jnp.where(lane == 0, rois, anchors)
    for q in range(4):
        keep_a[q, 6 * SUB :, :] = counts
        send_a[q, 6 * SUB :, :] = counts


def rpn_kernel(x, y, keep_b, send_b, keep_c, send_c, xp, gbuf):
    row = 32
    zero = jnp.zeros((row, C), jnp.bfloat16)
    for b in range(3):
        for j in (0, 49, 98):
            xp[b, j * row : (j + 1) * row, :] = zero
    at_col = lax.broadcasted_iota(jnp.int32, (row, C), 0)
    for i in range(2):

        def shift(r, carry):
            v = x[i, r]
            at = pl.multiple_of((i * 49 + 1 + r) * row, row)
            wide = v.astype(jnp.float32)
            left = jnp.where(at_col == 0, 0.0, pltpu.roll(wide, 1, 0))
            right = jnp.where(at_col == row - 1, 0.0, pltpu.roll(wide, row - 1, 0))
            xp[0, pl.ds(at, row), :] = left.astype(jnp.bfloat16)
            xp[1, pl.ds(at, row), :] = v
            xp[2, pl.ds(at, row), :] = right.astype(jnp.bfloat16)
            return carry

        lax.fori_loop(0, 48, shift, 0, unroll=8)
    where_b = block_id("y")
    where_c = block_id("z")
    for a in range(3):
        for b in range(3):
            t = 3 * a + b
            g = None
            for i in range(2):
                part = dot_t(
                    xp[b, (i * 49 + a) * row : (i * 49 + a + 48) * row, :],
                    y[i].reshape(48 * row, C),
                )
                g = part if g is None else g + part
            if t < 3:
                put(gbuf, g, where_b, keep_b, send_b, t)
            else:
                put(gbuf, g, where_c, keep_c, send_c, t - 3)


def whole():
    return pl.BlockSpec(memory_space=pltpu.VMEM)


def f32(*shape):
    return jax.ShapeDtypeStruct(shape, jnp.float32)


def mask_grads(roi, anchor, x, y):
    sm = pl.BlockSpec(memory_space=pltpu.SMEM)
    return pl.pallas_call(
        mask_kernel,
        name="mask_grads",
        out_shape=(f32(4, 200, C), f32(4, 200, C), f32(4, 96, C), f32(4, 96, C)),
        in_specs=[sm, sm, whole(), whole()],
        out_specs=[whole()] * 4,
        scratch_shapes=[
            VM((3, 31 * 112, C), jnp.bfloat16),
            VM((29 * 112, C), jnp.bfloat16),
            VM((C, C), jnp.float32),
        ],
        compiler_params=pltpu.CompilerParams(vmem_limit_bytes=24 << 20),
        cost_estimate=pl.CostEstimate(flops=3_700_000_000, bytes_accessed=6_000_000, transcendentals=0),
    )(roi, anchor, x, y)


def rpn_grads(x, y):
    return pl.pallas_call(
        rpn_kernel,
        name="rpn_grads",
        out_shape=(f32(4, 96, C), f32(4, 96, C), f32(4, 192, C), f32(4, 192, C)),
        in_specs=[whole(), whole()],
        out_specs=[whole()] * 4,
        scratch_shapes=[VM((3, 99 * 32, C), jnp.bfloat16), VM((C, C), jnp.float32)],
        compiler_params=pltpu.CompilerParams(vmem_limit_bytes=24 << 20),
        cost_estimate=pl.CostEstimate(flops=3_620_000_000, bytes_accessed=6_000_000, transcendentals=0),
    )(x, y)


def chain(keep, order):
    steps = [(axis, s) for axis in order for s in (0, 1)]
    for axis, s in steps[:2]:
        half = keep.shape[0] // 2
        keep = keep[:half] + swap(keep[half:], axis, s)
    for axis, s in steps[2:]:
        keep = keep + swap(keep, axis, s)
    for axis, s in reversed(steps[:2]):
        keep = jnp.concatenate([keep, swap(keep, axis, s)], 0)
    return keep, swap(keep, "core")


def update_kernel(a0, a1, b0, b1, c0, c1, mw, rw, mm, rm, nmw, nrw, nmm, nrm, gbuf):
    t = pl.program_id(0)
    ids = [block_id(axis) for axis in "xyz"]
    roi_total = a0[0, 192:200, 0:1][0:1, :]
    anchor_total = a0[0, 192:200, 1:2][0:1, :]

    def gather(own, other, which, slot):
        at = pl.multiple_of(slot * SUB, SUB)
        for q in range(4):
            mine, theirs = rows_of(ids[which], q)
            gbuf[mine, :] = own[q, pl.ds(at, SUB), :]
            gbuf[theirs, :] = other[q, pl.ds(at, SUB), :]

    @pl.when(t < 6)
    def _():
        gather(a0, a1, 0, t)

    @pl.when(t >= 6)
    def _():
        gather(b0, b1, 1, t - 6)

    moment = 0.9 * mm[...] + gbuf[...] / roi_total
    nmm[...] = moment
    nmw[...] = mw[...] - 0.02 * moment

    @pl.when(t < 3)
    def _():
        gather(b0, b1, 1, t + 3)

    @pl.when(t >= 3)
    def _():
        gather(c0, c1, 2, t - 3)

    moment = 0.9 * rm[...] + gbuf[...] / anchor_total
    nrm[...] = moment
    nrw[...] = rw[...] - 0.02 * moment


def update(chains, mw, rw, mm, rm):
    block = pl.BlockSpec((C, C), lambda t: (t, 0))
    return pl.pallas_call(
        update_kernel,
        name="update",
        grid=(9,),
        out_shape=tuple(f32(9 * C, C) for _ in range(4)),
        in_specs=[whole()] * 6 + [block] * 4,
        out_specs=[block] * 4,
        scratch_shapes=[VM((C, C), jnp.float32)],
        compiler_params=pltpu.CompilerParams(vmem_limit_bytes=20 << 20),
    )(*chains, mw, rw, mm, rm)


def on_device(mf, mc, roi, rf, rc, anchor, mw, rw, mm, rm):
    x = jnp.transpose(mf, (0, 2, 3, 1, 4)).reshape(2, 14, 112, C)
    y = jnp.transpose(mc, (0, 2, 3, 1, 4)).reshape(2, 14, 112, C)
    keep_a, send_a, keep_b, send_b = mask_grads(roi, anchor, x, y)
    keep_b2, send_b2, keep_c, send_c = rpn_grads(rf, rc)
    a = keep_a + swap(send_a, "core")
    b = keep_b + swap(send_b, "core")
    b2 = keep_b2 + swap(send_b2, "core")
    c = keep_c + swap(send_c, "core")
    ga = chain(a, ORDERS[0])
    gb = chain(jnp.concatenate([b, b2], 1), ORDERS[1])
    gc = chain(c, ORDERS[2])
    nmw, nrw, nmm, nrm = update(ga + gb + gc, mw, rw, mm, rm)
    return nmw, nrw, nmm, nrm


def solution(mesh):
    split = P(AXES)
    placed = (split,) * 6 + (P(),) * 4
    return jax.shard_map(
        on_device, mesh=mesh, in_specs=placed, out_specs=(P(),) * 4, check_vma=False
    )
```

```python
import functools

import jax
import jax.numpy as jnp
from jax import lax
from jax.experimental import pallas as pl
from jax.experimental.pallas import tpu as pltpu
from jax.sharding import PartitionSpec as P


AXES = ("gx", "gy")
DEVICES = 128
C = 256
SUB = 32
VM = pltpu.VMEM
HBM = pltpu.HBM

CHAINS = {
    "A": ("xyz", 0, (0, 3, 6, 1, 4, 7, 2), ()),
    "B": ("yzx", 1, (5, 8), (0, 3, 6, 1)),
    "C": ("zxy", 0, (), (4, 7, 2, 5, 8)),
}
SPLIT = 2


def coords(i):
    return {"x": i // 32, "core": (i // 16) % 2, "z": (i // 4) % 4, "y": i % 4}


def linear(d):
    return d["x"] * 32 + d["core"] * 16 + d["z"] * 4 + d["y"]


def partner(i, axis, step, lead):
    d = coords(i)
    half = (d["core"] + d["x"] + d["y"] + d["z"]) % 2
    if axis != "core":
        d[axis] ^= 1 if step == half ^ lead else 3
    d["core"] ^= 1
    return linear(d)


def swap(name, v, axis, step=0):
    pairs = [(i, partner(i, axis, step, CHAINS[name][1])) for i in range(DEVICES)]
    return lax.ppermute(v, AXES, pairs)


def block_id(name):
    order, lead = CHAINS[name][:2]
    gx, gy = lax.axis_index("gx"), lax.axis_index("gy")
    places = {"x": gx // 2, "z": gy // 4, "y": gy % 4}
    own = (gx + places["x"] + places["y"] + places["z"]) % 2
    at = places[order[0]]
    high = at // 2
    gray = (high + at) % 2
    one, two = gray * 2 + high, high * 2 + gray
    return (
        own * 4,
        (1 - own) * 4,
        jnp.where(own == lead, one, two),
        jnp.where(own == lead, two, one),
    )


def rows_of(where, q):
    base, partner_base, low, partner_low = where
    own = pl.multiple_of((base + (low ^ q)) * SUB, SUB)
    other = pl.multiple_of((partner_base + (partner_low ^ q)) * SUB, SUB)
    return pl.ds(own, SUB), pl.ds(other, SUB)


def put(buf, grad, where, keep, send, slot):
    buf[...] = grad
    for q in range(4):
        own, other = rows_of(where, q)
        keep[q, pl.ds(slot * SUB, SUB), :] = buf[own, :]
        send[q, pl.ds(slot * SUB, SUB), :] = buf[other, :]


def dot_t(a, b):
    return lax.dot_general(a, b, (((0,), (0,)), ((), ())), preferred_element_type=jnp.float32)


def columns_of(taps):
    return sorted({t % 3 for t in taps})


def load_mask(taps, roi, x, y, xp, yp):
    row = 14 * 8
    columns = columns_of(taps)
    zero = jnp.zeros((row, C), jnp.bfloat16)
    for k in range(len(columns)):
        for j in (0, 15, 30):
            xp[k, j * row : (j + 1) * row, :] = zero
    yp[14 * row : 15 * row, :] = zero
    slot = lax.broadcasted_iota(jnp.int32, (row, C), 0) % 8
    edge = jnp.zeros((8, C), jnp.bfloat16)
    for i in range(2):
        live = slot < roi[i]
        for r in range(14):
            v = x[i, r]
            shifted = (
                jnp.concatenate([edge, v[: row - 8]], 0),
                v,
                jnp.concatenate([v[8:], edge], 0),
            )
            at = (i * 15 + r + 1) * row
            for k, b in enumerate(columns):
                xp[k, at : at + row, :] = shifted[b]
            yp[at - row : at, :] = jnp.where(live, y[i, r], zero)


def mask_tap(t, taps, xp, yp):
    row, a, k = 14 * 8, t // 3, columns_of(taps).index(t % 3)
    return dot_t(xp[k, a * row : (a + 29) * row, :], yp[...])


def load_rpn(taps, x, xp):
    row = 32
    columns = columns_of(taps)
    zero = jnp.zeros((row, C), jnp.bfloat16)
    for k in range(len(columns)):
        for j in (0, 49, 98):
            xp[k, j * row : (j + 1) * row, :] = zero
    at_col = lax.broadcasted_iota(jnp.int32, (row, C), 0)
    for i in range(2):

        def shift(r, carry):
            v = x[i, r]
            at = pl.multiple_of((i * 49 + 1 + r) * row, row)
            wide = v.astype(jnp.float32)
            for k, b in enumerate(columns):
                if b == 1:
                    moved = v
                elif b == 0:
                    moved = jnp.where(at_col == 0, 0.0, pltpu.roll(wide, 1, 0))
                else:
                    moved = jnp.where(at_col == row - 1, 0.0, pltpu.roll(wide, row - 1, 0))
                xp[k, pl.ds(at, row), :] = moved.astype(jnp.bfloat16)
            return carry

        lax.fori_loop(0, 48, shift, 0, unroll=8)


def rpn_tap(t, taps, xp, y):
    row, a, k = 32, t // 3, columns_of(taps).index(t % 3)
    parts = [
        dot_t(
            xp[k, (i * 49 + a) * row : (i * 49 + a + 48) * row, :], y[i].reshape(48 * row, C)
        )
        for i in range(2)
    ]
    return parts[0] + parts[1]


def grads_mask_kernel(counts, x, y, keep_a, send_a, keep_b, send_b, xp, yp, buf):
    taps_a, taps_b = CHAINS["A"][2], CHAINS["B"][2]
    taps = taps_a + taps_b
    load_mask(taps, counts, x, y, xp, yp)
    where_a, where_b = block_id("A"), block_id("B")
    for k, t in enumerate(taps_a):
        put(buf, mask_tap(t, taps, xp, yp), where_a, keep_a, send_a, k)
    for k, t in enumerate(taps_b):
        put(buf, mask_tap(t, taps, xp, yp), where_b, keep_b, send_b, k)
    lane = lax.broadcasted_iota(jnp.int32, (8, C), 1)
    roi_sum = (counts[0] + counts[1]).astype(jnp.float32)
    anchor_sum = (counts[2] + counts[3]).astype(jnp.float32)
    sums = jnp.where(lane == 0, roi_sum, anchor_sum)
    for q in range(4):
        keep_a[q, len(taps_a) * SUB :, :] = sums
        send_a[q, len(taps_a) * SUB :, :] = sums


def grads_rpn_kernel(name, x, y, *refs):
    had, (keep, send, xp, buf) = refs[:-4], refs[-4:]
    rows = len(CHAINS[name][2]) * SUB
    if had:
        keep[:, :rows, :] = had[0][...]
        send[:, :rows, :] = had[1][...]
    taps = CHAINS[name][3]
    load_rpn(taps, x, xp)
    where = block_id(name)
    for k, t in enumerate(taps):
        put(buf, rpn_tap(t, taps, xp, y), where, keep, send, k + len(CHAINS[name][2]))


def whole():
    return pl.BlockSpec(memory_space=VM)


def f32(*shape):
    return jax.ShapeDtypeStruct(shape, jnp.float32)


def cost(mask, rpn):
    flops = 2 * C * C * (3136 * mask + 3072 * rpn)
    return pl.CostEstimate(flops=flops, bytes_accessed=4_000_000, transcendentals=0)


def grads_mask(roi, anchor, x, y):
    n_a, n_b = len(CHAINS["A"][2]), len(CHAINS["B"][2])
    shape_a, shape_b = f32(4, n_a * SUB + 8, C), f32(4, n_b * SUB, C)
    return pl.pallas_call(
        grads_mask_kernel,
        name="grads_a",
        out_shape=(shape_a, shape_a, shape_b, shape_b),
        in_specs=[pl.BlockSpec(memory_space=pltpu.SMEM)] + [whole()] * 2,
        out_specs=[whole()] * 4,
        scratch_shapes=[
            VM((3, 31 * 112, C), jnp.bfloat16),
            VM((29 * 112, C), jnp.bfloat16),
            VM((C, C), jnp.float32),
        ],
        compiler_params=pltpu.CompilerParams(vmem_limit_bytes=20 << 20),
        cost_estimate=cost(n_a + n_b, 0),
    )(jnp.concatenate([roi, anchor]), x, y)


def grads_rpn(name, x, y, had):
    rows = (len(CHAINS[name][2]) + len(CHAINS[name][3])) * SUB
    return pl.pallas_call(
        functools.partial(grads_rpn_kernel, name),
        out_shape=(f32(4, rows, C), f32(4, rows, C)),
        in_specs=[whole()] * (2 + len(had)),
        out_specs=[whole()] * 2,
        scratch_shapes=[
            VM((len(columns_of(CHAINS[name][3])), 99 * 32, C), jnp.bfloat16),
            VM((C, C), jnp.float32),
        ],
        compiler_params=pltpu.CompilerParams(vmem_limit_bytes=20 << 20),
        cost_estimate=cost(0, len(CHAINS[name][3])),
    )(x, y, *had)


def reduced(name, keep, send):
    keep = keep + swap(name, send, "core")
    steps = [(axis, s) for axis in CHAINS[name][0] for s in (0, 1)]
    for axis, s in steps[:SPLIT]:
        half = keep.shape[0] // 2
        keep = keep[:half] + swap(name, keep[half:], axis, s)
    for axis, s in steps[SPLIT:]:
        keep = keep + swap(name, keep, axis, s)
    for axis, s in reversed(steps[:SPLIT]):
        keep = jnp.concatenate([keep, swap(name, keep, axis, s)], 0)
    return keep, swap(name, keep, "core")


def update_kernel(name, taps, first, lane, own, other, counts, w, m, *refs):
    new_w, new_m, ow, om, buf, sem = refs[-6:]
    where = block_id(name)
    total = counts[0, 0:1, lane : lane + 1]
    copies = []
    for k, t in enumerate(taps):
        at = (first + k) * SUB
        for q in range(4):
            mine, theirs = rows_of(where, q)
            buf[mine, :] = own[q, at : at + SUB, :]
            buf[theirs, :] = other[q, at : at + SUB, :]
        rows = slice(t * C, (t + 1) * C)
        moment = 0.9 * m[rows, :] + buf[...] / total
        om[k] = moment
        ow[k] = w[rows, :] - 0.02 * moment
        copies.append(pltpu.make_async_copy(om.at[k], new_m.at[rows], sem.at[0, k]))
        copies.append(pltpu.make_async_copy(ow.at[k], new_w.at[rows], sem.at[1, k]))
        copies[-2].start()
        copies[-1].start()
    for c in copies:
        c.wait()


def update(name, taps, first, lane, own, other, counts, w, m, into):
    n = len(taps)
    return pl.pallas_call(
        functools.partial(update_kernel, name, taps, first, lane),
        out_shape=(f32(9 * C, C), f32(9 * C, C)),
        in_specs=[whole()] * 5 + [pl.BlockSpec(memory_space=HBM)] * len(into),
        out_specs=[pl.BlockSpec(memory_space=HBM)] * 2,
        scratch_shapes=[
            VM((n, C, C), jnp.float32),
            VM((n, C, C), jnp.float32),
            VM((C, C), jnp.float32),
            pltpu.SemaphoreType.DMA((2, n)),
        ],
        input_output_aliases={5: 0, 6: 1} if into else {},
        compiler_params=pltpu.CompilerParams(vmem_limit_bytes=8 << 20),
        cost_estimate=pl.CostEstimate(
            flops=1_000_000 * n, bytes_accessed=1_000_000 * n, transcendentals=0
        ),
    )(own, other, counts, w, m, *into)


def on_device(mf, mc, roi, rf, rc, anchor, mw, rw, mm, rm):
    x = jnp.transpose(mf, (0, 2, 3, 1, 4)).reshape(2, 14, 112, C)
    y = jnp.transpose(mc, (0, 2, 3, 1, 4)).reshape(2, 14, 112, C)
    *local_a, had_keep, had_send = grads_mask(roi, anchor, x, y)
    local_b = grads_rpn("B", rf, rc, (had_keep, had_send))
    local_c = grads_rpn("C", rf, rc, ())
    sums = {name: reduced(name, *local) for name, local in zip("ABC", (local_a, local_b, local_c))}
    counts = sums["A"][0][:1, len(CHAINS["A"][2]) * SUB :]
    new_mask, new_rpn = (), ()
    for name, (order, lead, mask_taps, rpn_taps) in CHAINS.items():
        own, other = sums[name]
        if mask_taps:
            new_mask = update(name, mask_taps, 0, 0, own, other, counts, mw, mm, new_mask)
        if rpn_taps:
            first = len(mask_taps)
            new_rpn = update(name, rpn_taps, first, 1, own, other, counts, rw, rm, new_rpn)
    return new_mask[0], new_rpn[0], new_mask[1], new_rpn[1]


def solution(mesh):
    split = P(AXES)
    placed = (split,) * 6 + (P(),) * 4
    return jax.shard_map(
        on_device, mesh=mesh, in_specs=placed, out_specs=(P(),) * 4, check_vma=False
    )
```
